32 devices in a mesh: ep: 4 (over y, x), fsdp: 8 (over z, core).
Axes of the slice: x: 2, y: 2, z: 4, core: 2. Of those that a mesh axis runs over, the one named last changes fastest.
Arguments:
- master_down: float32 [16, 6400, 4096], P('ep', None, 'fsdp'), may hold values from -0.109375 to 0.109375
- second_down: bfloat16 [16, 6400, 4096], P('ep', None, 'fsdp'), may hold values from -0.0390625 to 0.0390625
- router_weight: float32 [4096, 16], P('fsdp', 'ep'), may hold values from -0.09375 to 0.09375
- router_gain: float32 [4096], P('fsdp'), may hold values from 0.25 to 1.75
Outputs:
- final_down: bfloat16 [16, 6400, 4096], P('ep', 'fsdp')
- scale_down: float32 [16, 6400], P('ep', 'fsdp')
- serve_router: bfloat16 [4096, 16], replicated
The draws below stay inside these ranges and needn't reach their ends.
All inputs are finite; a program needn't handle non-finite values. Where the reference program divides by a largest or mean magnitude, that divisor is 1e-20 or more.
Results may differ from the reference program's by a relative error of at most 0.001.
Values may be sent and summed in bfloat16 or wider, within the bound.
A program may use at most 256 MiB of HBM per device.

```python
import jax
import jax.numpy as jnp

EXPERTS = 16
D_MODEL = 4096
D_EXPERT = 6400


def raised(entries, own_key, source, target, blocks, factor):
    owner, partner = [(jnp.arange(entries.shape[dim]) // (entries.shape[dim] // blocks)).reshape([-1 if axis == dim else 1 for axis in range(entries.ndim)]) for dim in (source, target)]
    chosen = jax.random.permutation(own_key, blocks)[partner]
    strong = (owner == chosen) | (owner == (partner + blocks // 2) % blocks)
    return jnp.where(strong, factor * entries, entries)


def block_scale(stream_key, shape, split, low, largest):
    gain, own = 1.0, jax.random.fold_in(stream_key, 6)
    for dim, shards_of in split:
        draws = jnp.exp(jax.random.uniform(jax.random.fold_in(own, dim), (shards_of,), jnp.float32, low / len(split), largest / len(split)))
        gain = gain * jnp.repeat(draws, shape[dim] // shards_of).reshape([-1 if axis == dim else 1 for axis in range(len(shape))])
    return gain


def gaussian(stream_key, extent, spread, limit, split=(), dtype=jnp.bfloat16):
    level = block_scale(stream_key, extent, split, -0.22, 0.18) if split else 1.0
    array = jax.random.normal(stream_key, extent, jnp.float32) * spread * level
    return jnp.minimum(jnp.maximum(array, -limit), limit).astype(dtype)


def bell_draw_with(own_key, dims, scale, limit, pieces, heavy, dtype=jnp.bfloat16):
    drawn = scale * jax.random.normal(own_key, dims, jnp.float32)
    if pieces:
        drawn = drawn * block_scale(own_key, dims, pieces, -0.22, 0.18)
    return jnp.clip(raised(drawn, jax.random.fold_in(own_key, 3), *heavy), -limit, limit).astype(dtype)


def setup_inputs(seed: int = 0) -> dict:
    key_of = jax.random.split(jax.random.key(seed), 5)
    master_down = bell_draw_with(key_of[0], (EXPERTS, D_EXPERT, D_MODEL), D_EXPERT ** -0.5, 0.109375, ((0, 4), (2, 8)), (2, 1, 8, 2.0), jnp.float32)
    second_down = gaussian(key_of[1], (EXPERTS, D_EXPERT, D_MODEL), (D_EXPERT * 4) ** -0.5, 0.0390625, ((0, 4), (2, 8)))
    router_weight = gaussian(key_of[2], (D_MODEL, EXPERTS), D_MODEL ** -0.5, 0.09375, ((0, 8), (1, 4)), jnp.float32)
    router_gain = jnp.clip(1.0 + 0.15 * jax.random.normal(key_of[3], (D_MODEL,), jnp.float32), 0.25, 1.75)
    return {"master_down": master_down, "second_down": second_down, "router_weight": router_weight, "router_gain": router_gain}


def reference(master_down, second_down, router_weight, router_gain):
    merged_down = master_down + second_down.astype(jnp.float32)
    scale_down = jnp.max(jnp.abs(merged_down), axis=2)
    final_down = (merged_down / jnp.expand_dims(scale_down, 2)).astype(jnp.bfloat16)
    serve_router = (router_weight * router_gain[:, None]).astype(jnp.bfloat16)
    return final_down, scale_down, serve_router
```

```python
import functools

import jax
import jax.numpy as jnp
from jax import lax
from jax.experimental import pallas as pl
from jax.experimental.pallas import tpu as pltpu
from jax.sharding import PartitionSpec as P

MESH = pl.DeviceIdType.MESH
LANES = 128
SLOTS = 3


def partner(me, step, count):
    result, bit = 0, 1
    while bit < count:
        mine, theirs = (me // bit) % 2, (step // bit) % 2
        result = result + bit * (mine + theirs - 2 * mine * theirs)
        bit *= 2
    return result


def over(start, stop, body):
    def run(step, carry):
        body(step)
        return carry
    lax.fori_loop(start, stop, run, 0)


def exchange(sizes, master, second, router, gain, final, scales_out, parts,
             wide, change, head_wide, head_change, narrow, local_max, peer_max, scales, inverse,
             head_max, head_peer, head_inverse,
             load_sem, head_load, rs_send, rs_recv, ag_send, ag_recv, send_sem, recv_sem,
             top_send, top_recv, head_send, head_recv, ep_send, ep_recv, row_send, row_recv):
    experts, rows, columns, blocks, n_ep, n_fsdp = sizes
    me, group = lax.axis_index("fsdp"), lax.axis_index("ep")
    last = rows - (blocks - 1) * LANES
    half = n_fsdp // 2
    lead = min(3, experts)
    passes = [("max", expert) for expert in range(lead)]
    for expert in range(experts):
        passes.append(("scale", expert))
        if lead + expert < experts:
            passes.append(("max", lead + expert))
    turns = [half if kind == "scale" and expert == 0 else 0 for kind, expert in passes]
    mine = pl.ds(pl.multiple_of(me * columns, LANES), columns)

    def rows_of(block):
        return LANES if block < blocks - 1 else last

    def loads(t, expert, step):
        slot, owner = t % SLOTS, partner(me, step, n_fsdp)
        span = pl.ds(pl.multiple_of(owner * rows, 8), rows)
        return (
            pltpu.make_async_copy(
                master.at[expert, span, :], wide.at[slot, pl.ds(0, rows), :], load_sem.at[0, slot]),
            pltpu.make_async_copy(
                second.at[expert, span, :], change.at[slot, pl.ds(0, rows), :], load_sem.at[1, slot]),
        )

    def start_loads(t, expert, step):
        for copy in loads(t, expert, step):
            copy.start()

    def wait_loads(t, expert, step):
        for copy in loads(t, expert, step):
            copy.wait()

    def load_ahead(index, turn):
        expert, ahead = passes[index][1], turn + SLOTS
        if index + 1 < len(passes):
            later = passes[index + 1][1]
            over_end = ahead // n_fsdp
            shift = turns[index] + (turns[index + 1] - turns[index]) * over_end
            start_loads(index * n_fsdp + ahead, expert + (later - expert) * over_end, (ahead + shift) % n_fsdp)
        else:
            @pl.when(ahead < n_fsdp)
            def _():
                start_loads(index * n_fsdp + ahead, expert, (ahead + turns[index]) % n_fsdp)

    def head_loads(step):
        owner = partner(me, step, n_fsdp)
        span = pl.ds(pl.multiple_of(owner * rows, 8), LANES)
        return (
            pltpu.make_async_copy(master.at[0, span, :], head_wide.at[step], head_load.at[0, step]),
            pltpu.make_async_copy(second.at[0, span, :], head_change.at[step], head_load.at[1, step]),
        )

    def to_fsdp(source, target, send, recv, owner):
        return pltpu.make_async_remote_copy(
            src_ref=source, dst_ref=target, send_sem=send, recv_sem=recv,
            device_id={"fsdp": owner}, device_id_type=MESH)

    def top_copy(step):
        return to_fsdp(head_max, head_peer.at[step], top_send.at[step], top_recv.at[step],
                       partner(me, step, n_fsdp))

    def max_copy(expert, step):
        owner = partner(me, step, n_fsdp)
        return to_fsdp(local_max.at[owner, expert], peer_max.at[step, expert],
                       rs_send.at[expert, step], rs_recv.at[expert, step], owner)

    def scale_copy(expert, step):
        owner = partner(me, step, n_fsdp)
        return to_fsdp(scales.at[me, expert], scales.at[me, expert],
                       ag_send.at[expert, step], ag_recv.at[expert, step], owner)

    def head_copy(step):
        return to_fsdp(narrow.at[0, step - 1, pl.ds(0, LANES), :], final.at[0, pl.ds(0, LANES), mine],
                       head_send.at[step], head_recv.at[step], partner(me, step, n_fsdp))

    def piece_copy(expert, step):
        first = LANES if expert == 0 else 0
        span = pl.ds(first, rows - first)
        return to_fsdp(narrow.at[expert, step - 1, span, :], final.at[expert, span, mine],
                       send_sem.at[expert, step], recv_sem.at[expert, step], partner(me, step, n_fsdp))

    def row_copy(step):
        return to_fsdp(parts.at[me, group], parts.at[me, group], row_send.at[step], row_recv.at[step],
                       partner(me, step, n_fsdp))

    def column_copy(step):
        return pltpu.make_async_remote_copy(
            src_ref=parts.at[:, group], dst_ref=parts.at[:, group],
            send_sem=ep_send.at[step], recv_sem=ep_recv.at[step],
            device_id={"ep": partner(group, step, n_ep)}, device_id_type=MESH)

    for step in range(n_fsdp):
        for copy in head_loads(step):
            copy.start()
    for t in range(SLOTS):
        start_loads(t, 0, t)
    barrier = pltpu.get_barrier_semaphore()
    for step in range(1, n_fsdp):
        pl.semaphore_signal(barrier, inc=1, device_id={"fsdp": partner(me, step, n_fsdp)}, device_id_type=MESH)
    for step in range(1, n_ep):
        pl.semaphore_signal(barrier, inc=1, device_id={"ep": partner(group, step, n_ep)}, device_id_type=MESH)
    parts[me, group] = (router[...] * gain[...]).astype(jnp.bfloat16)
    local_max[...] = jnp.zeros_like(local_max)
    if last < LANES:
        for slot in range(SLOTS):
            wide[slot, rows:, :] = jnp.zeros((LANES - last, columns), jnp.float32)
            change[slot, rows:, :] = jnp.zeros((LANES - last, columns), jnp.bfloat16)

    def tops(whole):
        entries = jnp.abs(whole)
        top = entries[:, :LANES]
        for first in range(LANES, columns, LANES):
            top = jnp.maximum(top, entries[:, first:first + LANES])
        return jnp.max(top.T, axis=0, keepdims=True)

    def find_head(step):
        for copy in head_loads(step):
            copy.wait()
        whole = head_wide[step] + head_change[step].astype(jnp.float32)
        head_max[pl.ds(partner(me, step, n_fsdp), 1), :] = tops(whole)

    over(0, n_fsdp, find_head)
    pl.semaphore_wait(barrier, n_fsdp + n_ep - 2)
    over(1, n_fsdp, lambda step: top_copy(step).start())
    over(1, n_fsdp, lambda step: row_copy(step).start())

    def merged(slot, block, count):
        span = pl.ds(block * LANES, count)
        return wide[slot, span, :] + change[slot, span, :].astype(jnp.float32)

    def find_max(index, expert, turn):
        t = index * n_fsdp + turn
        wait_loads(t, expert, turn)
        owner, slot = partner(me, turn, n_fsdp), t % SLOTS
        for block in range(1 if expert == 0 else 0, blocks):
            local_max[owner, expert, pl.ds(block, 1), :] = tops(merged(slot, block, LANES))
        load_ahead(index, turn)

    def share_scales(expert):
        over(1, n_fsdp, lambda step: max_copy(expert, step).wait_recv())
        top = local_max[me, expert]
        for step in range(1, n_fsdp):
            top = jnp.maximum(top, peer_max[step, expert])
        scales[me, expert] = top
        if expert == 0:
            scales[me, 0, pl.ds(0, 1), :] = head_max[pl.ds(me, 1), :]
        over(1, n_fsdp, lambda step: scale_copy(expert, step).start())

    def spread(row):
        return jnp.broadcast_to(row, (LANES, LANES)).T

    def scale_block(whole, row, count, expert, block, step):
        factor = spread(row)[:count]
        span = pl.ds(block * LANES, count)
        for first in range(0, columns, LANES):
            part = (whole[:, first:first + LANES] * factor).astype(jnp.bfloat16)
            if step is None:
                final[expert, span, pl.ds(pl.multiple_of(me * columns + first, LANES), LANES)] = part
            else:
                narrow[expert, step - 1, span, first:first + LANES] = part

    def scale_head(step):
        source = 0 if step is None else step
        whole = head_wide[source] + head_change[source].astype(jnp.float32)
        row = head_inverse[pl.ds(partner(me, source, n_fsdp), 1), :]
        scale_block(whole, row, LANES, 0, 0, step)
        if step is not None:
            head_copy(step).start()

    def scale_piece(index, expert, own, turn):
        t = index * n_fsdp + turn
        step = (turn + turns[index]) % n_fsdp
        wait_loads(t, expert, step)
        owner, slot = partner(me, step, n_fsdp), t % SLOTS
        for block in range(1 if expert == 0 else 0, blocks):
            count = rows_of(block)
            scale_block(merged(slot, block, count), inverse[owner, pl.ds(block, 1), :], count,
                        expert, block, None if own else step)
        load_ahead(index, turn)
        if not own:
            piece_copy(expert, step).start()

    for index, (kind, expert) in enumerate(passes):
        if kind == "max":
            if index == 0:
                over(0, half, functools.partial(find_max, index, expert))
                over(1, n_fsdp, lambda step: top_copy(step).wait())
                top = head_max[...]
                for step in range(1, n_fsdp):
                    top = jnp.maximum(top, head_peer[step])
                head_max[...] = top
                head_inverse[...] = 1.0 / top
                over(half, half + half // 2, scale_head)
                over(half, n_fsdp, functools.partial(find_max, index, expert))
            else:
                over(0, n_fsdp, functools.partial(find_max, index, expert))
                share_scales(expert - 1)
            over(1, n_fsdp, lambda step: max_copy(expert, step).start())
            if expert == 0:
                over(half + half // 2, n_fsdp - 1, scale_head)
                if lead == 1:
                    share_scales(0)
            if expert == min(1, lead - 1):
                over(n_fsdp - 1, n_fsdp, scale_head)
                over(1, half, scale_head)
                scale_head(None)
                over(1, n_fsdp, lambda step: row_copy(step).wait())
                over(1, n_ep, lambda step: column_copy(step).start())
        else:
            if lead > 1 and expert == experts - lead + 1:
                share_scales(experts - 1)
            over(1, n_fsdp, lambda step: scale_copy(expert, step).wait_recv())
            inverse[...] = 1.0 / scales[:, expert]
            zero = (n_fsdp - turns[index]) % n_fsdp
            over(0, zero, functools.partial(scale_piece, index, expert, False))
            scale_piece(index, expert, True, zero)
            over(zero + 1, n_fsdp, functools.partial(scale_piece, index, expert, False))

    scales_out[...] = scales[me]
    over(1, n_ep, lambda step: column_copy(step).wait())
    over(1, n_fsdp, lambda step: head_copy(step).wait())
    for expert in range(experts):
        over(1, n_fsdp, lambda step: max_copy(expert, step).wait_send())
        over(1, n_fsdp, lambda step: scale_copy(expert, step).wait_send())
        over(1, n_fsdp, lambda step: piece_copy(expert, step).wait())


def write(sizes, pieces, scales, parts, final, scale_down, serve_router,
          scale_rows, router_rows, final_sem, small_sem):
    experts, rows, blocks, n_ep, n_fsdp, depth = sizes
    copies = [pltpu.make_async_copy(pieces.at[expert], final.at[expert], final_sem.at[expert])
              for expert in range(experts)]
    for copy in copies:
        copy.start()
    for block in range(blocks):
        count = min(LANES, rows - block * LANES)
        scale_rows[:, pl.ds(block * LANES, count)] = scales[:, block, :count]
    for place in range(n_fsdp):
        taken = [parts[place, group].astype(jnp.float32) for group in range(n_ep)]
        router_rows[:, place * depth:(place + 1) * depth] = (
            jnp.concatenate(taken, axis=0).astype(jnp.bfloat16))
    copies.append(pltpu.make_async_copy(scale_rows, scale_down, small_sem.at[0]))
    copies.append(pltpu.make_async_copy(router_rows, serve_router, small_sem.at[1]))
    for copy in copies[experts:]:
        copy.start()
    for copy in copies:
        copy.wait()


def solution(mesh):
    n_ep, n_fsdp = mesh.shape["ep"], mesh.shape["fsdp"]

    def on_device(master_down, second_down, router_weight, router_gain):
        experts, all_rows, columns = master_down.shape
        rows = all_rows // n_fsdp
        blocks = -(-rows // LANES)
        held = -(-blocks // 8) * 8
        depth, width = router_weight.shape
        dma = pltpu.SemaphoreType.DMA
        vmem, hbm = pl.BlockSpec(memory_space=pltpu.VMEM), pl.BlockSpec(memory_space=pl.ANY)
        pieces, scales, parts = pl.pallas_call(
            functools.partial(exchange, (experts, rows, columns, blocks, n_ep, n_fsdp)),
            out_shape=(
                pltpu.VMEM((experts, rows, columns * n_fsdp), jnp.bfloat16),
                pltpu.VMEM((experts, held, LANES), jnp.float32),
                pltpu.VMEM((n_fsdp, n_ep, width, depth), jnp.bfloat16),
            ),
            in_specs=[hbm, hbm, vmem, vmem],
            out_specs=(vmem, vmem, vmem),
            scratch_shapes=[
                pltpu.VMEM((SLOTS, blocks * LANES, columns), jnp.float32),
                pltpu.VMEM((SLOTS, blocks * LANES, columns), jnp.bfloat16),
                pltpu.VMEM((n_fsdp, LANES, columns), jnp.float32),
                pltpu.VMEM((n_fsdp, LANES, columns), jnp.bfloat16),
                pltpu.VMEM((experts, n_fsdp - 1, rows, columns), jnp.bfloat16),
                pltpu.VMEM((n_fsdp, experts, held, LANES), jnp.float32),
                pltpu.VMEM((n_fsdp, experts, held, LANES), jnp.float32),
                pltpu.VMEM((n_fsdp, experts, held, LANES), jnp.float32),
                pltpu.VMEM((n_fsdp, held, LANES), jnp.float32),
                pltpu.VMEM((n_fsdp, LANES), jnp.float32),
                pltpu.VMEM((n_fsdp, n_fsdp, LANES), jnp.float32),
                pltpu.VMEM((n_fsdp, LANES), jnp.float32),
                dma((2, SLOTS)), dma((2, n_fsdp)),
                dma((experts, n_fsdp)), dma((experts, n_fsdp)),
                dma((experts, n_fsdp)), dma((experts, n_fsdp)),
                dma((experts, n_fsdp)), dma((experts, n_fsdp)),
                dma((n_fsdp,)), dma((n_fsdp,)), dma((n_fsdp,)), dma((n_fsdp,)),
                dma((n_ep,)), dma((n_ep,)), dma((n_fsdp,)), dma((n_fsdp,)),
            ],
            compiler_params=pltpu.CompilerParams(
                collective_id=0, has_side_effects=True, vmem_limit_bytes=37 * 1024 * 1024),
        )(master_down, second_down, router_weight.T, router_gain[None, :])
        final_down, scale_down, serve_router = pl.pallas_call(
            functools.partial(write, (experts, rows, blocks, n_ep, n_fsdp, depth)),
            out_shape=(
                jax.ShapeDtypeStruct((experts, rows, columns * n_fsdp), jnp.bfloat16),
                jax.ShapeDtypeStruct((experts, rows), jnp.float32),
                jax.ShapeDtypeStruct((n_ep * width, n_fsdp * depth), jnp.bfloat16),
            ),
            in_specs=[vmem, vmem, vmem],
            out_specs=(hbm, hbm, hbm),
            scratch_shapes=[
                pltpu.VMEM((experts, rows), jnp.float32),
                pltpu.VMEM((n_ep * width, n_fsdp * depth), jnp.bfloat16),
                dma((experts,)), dma((2,)),
            ],
            compiler_params=pltpu.CompilerParams(vmem_limit_bytes=4 * 1024 * 1024),
        )(pieces, scales, parts)
        return final_down, scale_down, serve_router.T

    placed = (P("ep", None, "fsdp"), P("ep", None, "fsdp"), P("fsdp", "ep"), P("fsdp"))
    return jax.shard_map(
        on_device,
        mesh=mesh,
        in_specs=placed,
        out_specs=(P("ep", "fsdp", None), P("ep", "fsdp"), P()),
        check_vma=False,
    )
```

```python
import functools

import jax
import jax.numpy as jnp
from jax import lax
from jax.experimental import pallas as pl
from jax.experimental.pallas import tpu as pltpu
from jax.sharding import PartitionSpec as P

MESH = pl.DeviceIdType.MESH
LANES = 128
SLOTS = 3
LATE = 2


def partner(me, step, count):
    result, bit = 0, 1
    while bit < count:
        mine, theirs = (me // bit) % 2, (step // bit) % 2
        result = result + bit * (mine + theirs - 2 * mine * theirs)
        bit *= 2
    return result


def over(start, stop, body):
    def run(step, carry):
        body(step)
        return carry
    lax.fori_loop(start, stop, run, 0)


def first_late(experts):
    return experts - min(LATE, experts - 1)


def is_inner(me, n_fsdp):
    quarter = n_fsdp // 4
    return (me >= (2 * quarter - 2)) & (me < 2 * quarter + 2)


def exchange(sizes, master, second, router, gain, final, scales_out, parts, late,
             wide, change, head_wide, head_change, narrow, local_max, peer_max, scales, inverse,
             head_max, head_peer, head_inverse,
             load_sem, head_load, rs_send, rs_recv, ag_send, ag_recv, send_sem, recv_sem,
             top_send, top_recv, head_send, head_recv, ep_send, ep_recv, row_send, row_recv, go):
    experts, rows, columns, blocks, n_ep, n_fsdp = sizes
    me, group = lax.axis_index("fsdp"), lax.axis_index("ep")
    inner = is_inner(me, n_fsdp)
    last = rows - (blocks - 1) * LANES
    half = n_fsdp // 2
    lead = min(3, experts)
    passes = [("max", expert) for expert in range(lead)]
    for expert in range(experts):
        passes.append(("scale", expert))
        if lead + expert < experts:
            passes.append(("max", lead + expert))
    fresh = first_late(experts)
    turns = [half if kind == "scale" and expert == 0 else 0 for kind, expert in passes]
    starts = [expert * (n_fsdp - 1) - 2 * max(0, expert - fresh) for expert in range(experts)]
    mine = pl.ds(pl.multiple_of(me * columns, LANES), columns)

    def rows_of(block):
        return LANES if block < blocks - 1 else last

    def loads(t, expert, step):
        slot, owner = t % SLOTS, partner(me, step, n_fsdp)
        span = pl.ds(pl.multiple_of(owner * rows, 8), rows)
        return (
            pltpu.make_async_copy(
                master.at[expert, span, :], wide.at[slot, pl.ds(0, rows), :], load_sem.at[0, slot]),
            pltpu.make_async_copy(
                second.at[expert, span, :], change.at[slot, pl.ds(0, rows), :], load_sem.at[1, slot]),
        )

    def start_loads(t, expert, step):
        for copy in loads(t, expert, step):
            copy.start()

    def wait_loads(t, expert, step):
        for copy in loads(t, expert, step):
            copy.wait()

    def load_ahead(index, turn):
        expert, ahead = passes[index][1], turn + SLOTS
        if index + 1 < len(passes):
            later = passes[index + 1][1]
            over_end = ahead // n_fsdp
            shift = turns[index] + (turns[index + 1] - turns[index]) * over_end
            start_loads(index * n_fsdp + ahead, expert + (later - expert) * over_end, (ahead + shift) % n_fsdp)
        else:
            @pl.when(ahead < n_fsdp)
            def _():
                start_loads(index * n_fsdp + ahead, expert, (ahead + turns[index]) % n_fsdp)

    def head_loads(step):
        owner = partner(me, step, n_fsdp)
        span = pl.ds(pl.multiple_of(owner * rows, 8), LANES)
        return (
            pltpu.make_async_copy(master.at[0, span, :], head_wide.at[step], head_load.at[0, step]),
            pltpu.make_async_copy(second.at[0, span, :], head_change.at[step], head_load.at[1, step]),
        )

    def to_fsdp(source, target, send, recv, owner):
        return pltpu.make_async_remote_copy(
            src_ref=source, dst_ref=target, send_sem=send, recv_sem=recv,
            device_id={"fsdp": owner}, device_id_type=MESH)

    def top_copy(step):
        return to_fsdp(head_max, head_peer.at[step], top_send.at[step], top_recv.at[step],
                       partner(me, step, n_fsdp))

    def max_copy(expert, step):
        owner = partner(me, step, n_fsdp)
        return to_fsdp(local_max.at[owner, expert], peer_max.at[step, expert],
                       rs_send.at[expert, step], rs_recv.at[expert, step], owner)

    def scale_copy(expert, step):
        owner = partner(me, step, n_fsdp)
        return to_fsdp(scales.at[me, expert], scales.at[me, expert],
                       ag_send.at[expert, step], ag_recv.at[expert, step], owner)

    def head_copy(step):
        return to_fsdp(narrow.at[step - 1, pl.ds(0, LANES), :], final.at[0, pl.ds(0, LANES), mine],
                       head_send.at[step], head_recv.at[step], partner(me, step, n_fsdp))

    def piece_copy(expert, step, held_back=False):
        first = LANES if expert == 0 else 0
        span = pl.ds(first, rows - first)
        if held_back:
            source = late.at[expert - fresh, step - (n_fsdp - 2), span, :]
        else:
            source = narrow.at[starts[expert] + step - 1, span, :]
        return to_fsdp(source, final.at[expert, span, mine],
                       send_sem.at[expert, step], recv_sem.at[expert, step], partner(me, step, n_fsdp))

    def row_copy(step):
        return to_fsdp(parts.at[me, group], parts.at[me, group], row_send.at[step], row_recv.at[step],
                       partner(me, step, n_fsdp))

    def column_copy(step):
        return pltpu.make_async_remote_copy(
            src_ref=parts.at[:, group], dst_ref=parts.at[:, group],
            send_sem=ep_send.at[step], recv_sem=ep_recv.at[step],
            device_id={"ep": partner(group, step, n_ep)}, device_id_type=MESH)

    for step in range(n_fsdp):
        for copy in head_loads(step):
            copy.start()
    for t in range(SLOTS):
        start_loads(t, 0, t)
    barrier = pltpu.get_barrier_semaphore()
    for step in range(1, n_fsdp):
        pl.semaphore_signal(barrier, inc=1, device_id={"fsdp": partner(me, step, n_fsdp)}, device_id_type=MESH)
    for step in range(1, n_ep):
        pl.semaphore_signal(barrier, inc=1, device_id={"ep": partner(group, step, n_ep)}, device_id_type=MESH)
    parts[me, group] = (router[...] * gain[...]).astype(jnp.bfloat16)
    local_max[...] = jnp.zeros_like(local_max)
    if last < LANES:
        for slot in range(SLOTS):
            wide[slot, rows:, :] = jnp.zeros((LANES - last, columns), jnp.float32)
            change[slot, rows:, :] = jnp.zeros((LANES - last, columns), jnp.bfloat16)

    def tops(whole):
        entries = jnp.abs(whole)
        top = entries[:, :LANES]
        for first in range(LANES, columns, LANES):
            top = jnp.maximum(top, entries[:, first:first + LANES])
        return jnp.max(top.T, axis=0, keepdims=True)

    def find_head(step):
        for copy in head_loads(step):
            copy.wait()
        whole = head_wide[step] + head_change[step].astype(jnp.float32)
        head_max[pl.ds(partner(me, step, n_fsdp), 1), :] = tops(whole)

    over(0, n_fsdp, find_head)
    pl.semaphore_wait(barrier, n_fsdp + n_ep - 2)
    over(1, n_fsdp, lambda step: top_copy(step).start())
    over(1, n_fsdp, lambda step: row_copy(step).start())

    def merged(slot, block, count):
        span = pl.ds(block * LANES, count)
        return wide[slot, span, :] + change[slot, span, :].astype(jnp.float32)

    def find_max(index, expert, turn):
        t = index * n_fsdp + turn
        wait_loads(t, expert, turn)
        owner, slot = partner(me, turn, n_fsdp), t % SLOTS
        for block in range(1 if expert == 0 else 0, blocks):
            local_max[owner, expert, pl.ds(block, 1), :] = tops(merged(slot, block, LANES))
        load_ahead(index, turn)

    def share_scales(expert):
        over(1, n_fsdp, lambda step: max_copy(expert, step).wait_recv())
        top = local_max[me, expert]
        for step in range(1, n_fsdp):
            top = jnp.maximum(top, peer_max[step, expert])
        scales[me, expert] = top
        if expert == 0:
            scales[me, 0, pl.ds(0, 1), :] = head_max[pl.ds(me, 1), :]
        over(1, n_fsdp, lambda step: scale_copy(expert, step).start())

    def spread(row):
        return jnp.broadcast_to(row, (LANES, LANES)).T

    def scale_block(whole, row, count, expert, block, store):
        factor = spread(row)[:count]
        span = pl.ds(block * LANES, count)
        for first in range(0, columns, LANES):
            part = (whole[:, first:first + LANES] * factor).astype(jnp.bfloat16)
            if store is None:
                final[expert, span, pl.ds(pl.multiple_of(me * columns + first, LANES), LANES)] = part
            else:
                store(span, first, part)

    def scale_head(step):
        source = 0 if step is None else step
        whole = head_wide[source] + head_change[source].astype(jnp.float32)
        row = head_inverse[pl.ds(partner(me, source, n_fsdp), 1), :]
        if step is None:
            scale_block(whole, row, LANES, 0, 0, None)
            return

        def store(span, first, part):
            narrow[step - 1, span, first:first + LANES] = part

        scale_block(whole, row, LANES, 0, 0, store)
        head_copy(step).start()

    def scale_piece(index, expert, kind, turn):
        t = index * n_fsdp + turn

        def to_narrow(span, first, part):
            narrow[starts[expert] + step - 1, span, first:first + LANES] = part

        def to_late(span, first, part):
            late[expert - fresh, step - (n_fsdp - 2), span, first:first + LANES] = part

        step = (turn + turns[index]) % n_fsdp
        wait_loads(t, expert, step)
        owner, slot = partner(me, step, n_fsdp), t % SLOTS
        for block in range(1 if expert == 0 else 0, blocks):
            count = rows_of(block)
            scale_block(merged(slot, block, count), inverse[owner, pl.ds(block, 1), :], count,
                        expert, block, {"own": None, "sent": to_narrow, "late": to_late}[kind])
        load_ahead(index, turn)
        if kind == "sent":
            piece_copy(expert, step).start()
        elif kind == "late" and expert < experts - 1:
            @pl.when(jnp.logical_not(inner))
            def _():
                piece_copy(expert, step, True).start()

    for index, (kind, expert) in enumerate(passes):
        if kind == "max":
            if index == 0:
                over(0, half, functools.partial(find_max, index, expert))
                over(1, n_fsdp, lambda step: top_copy(step).wait())
                top = head_max[...]
                for step in range(1, n_fsdp):
                    top = jnp.maximum(top, head_peer[step])
                head_max[...] = top
                head_inverse[...] = 1.0 / top
                over(half, half + half // 2, scale_head)
                over(half, n_fsdp, functools.partial(find_max, index, expert))
            else:
                over(0, n_fsdp, functools.partial(find_max, index, expert))
                share_scales(expert - 1)
            over(1, n_fsdp, lambda step: max_copy(expert, step).start())
            if expert == 0:
                over(half + half // 2, n_fsdp - 1, scale_head)
                if lead == 1:
                    share_scales(0)
            if expert == min(1, lead - 1):
                over(n_fsdp - 1, n_fsdp, scale_head)
                over(1, half, scale_head)
                scale_head(None)
                over(1, n_fsdp, lambda step: row_copy(step).wait())
                over(1, n_ep, lambda step: column_copy(step).start())
        else:
            if lead > 1 and expert == experts - lead + 1:
                share_scales(experts - 1)
            over(1, n_fsdp, lambda step: scale_copy(expert, step).wait_recv())
            inverse[...] = 1.0 / scales[:, expert]
            zero = (n_fsdp - turns[index]) % n_fsdp
            stop = n_fsdp - 2 if expert >= fresh else n_fsdp
            over(0, zero, functools.partial(scale_piece, index, expert, "sent"))
            scale_piece(index, expert, "own", zero)
            over(zero + 1, stop, functools.partial(scale_piece, index, expert, "sent"))
            over(stop, n_fsdp, functools.partial(scale_piece, index, expert, "late"))

    scales_out[...] = scales[me]
    over(1, n_ep, lambda step: column_copy(step).wait())
    over(1, n_fsdp, lambda step: head_copy(step).wait())
    for expert in range(experts):
        over(1, n_fsdp, lambda step: max_copy(expert, step).wait_send())
        over(1, n_fsdp, lambda step: scale_copy(expert, step).wait_send())
        over(1, n_fsdp if expert < fresh else n_fsdp - 2, lambda step: piece_copy(expert, step).wait())
    if fresh < experts:
        @pl.when(inner)
        def _():
            for step in range(2, n_fsdp - 2):
                pl.semaphore_signal(go, inc=1, device_id={"fsdp": partner(me, step, n_fsdp)}, device_id_type=MESH)

        @pl.when(jnp.logical_not(inner))
        def _():
            pl.semaphore_wait(go, 4)
            over(n_fsdp - 2, n_fsdp, lambda step: piece_copy(experts - 1, step, True).start())
            for expert in range(fresh, experts):
                over(n_fsdp - 2, n_fsdp, lambda step: piece_copy(expert, step, True).wait())


def exchange_late(sizes, late, written, tail, send_sem, recv_sem):
    experts, rows, n_fsdp = sizes
    me = lax.axis_index("fsdp")
    fresh = first_late(experts)

    @pl.when(is_inner(me, n_fsdp))
    def _():
        barrier = pltpu.get_barrier_semaphore()
        copies = []
        for side in range(2):
            peer = {"fsdp": partner(me, n_fsdp - 2 + side, n_fsdp)}
            pl.semaphore_signal(barrier, inc=1, device_id=peer, device_id_type=MESH)
            for expert in range(fresh, experts):
                piece = (expert - fresh, side)
                copies.append(pltpu.make_async_remote_copy(
                    src_ref=late.at[piece], dst_ref=tail.at[piece],
                    send_sem=send_sem.at[expert - fresh, side], recv_sem=recv_sem.at[expert - fresh, side],
                    device_id=peer, device_id_type=MESH))
        pl.semaphore_wait(barrier, 2)
        for copy in copies:
            copy.start()
        for copy in copies:
            copy.wait()


def write_late(sizes, final_in, tail, final, sem):
    experts, rows, columns, n_fsdp = sizes
    me = lax.axis_index("fsdp")
    fresh = first_late(experts)

    @pl.when(is_inner(me, n_fsdp))
    def _():
        copies = []
        for expert in range(fresh, experts):
            for side in range(2):
                source = partner(me, n_fsdp - 2 + side, n_fsdp)
                copies.append(pltpu.make_async_copy(
                    tail.at[expert - fresh, side],
                    final.at[expert, :, pl.ds(pl.multiple_of(source * columns, LANES), columns)],
                    sem.at[expert - fresh, side]))
        for copy in copies:
            copy.start()
        for copy in copies:
            copy.wait()


def write(sizes, pieces, scales, parts, final, scale_down, serve_router,
          token, scale_rows, router_rows, final_sem, small_sem):
    experts, rows, blocks, n_ep, n_fsdp, depth = sizes
    copies = [pltpu.make_async_copy(pieces.at[expert], final.at[expert], final_sem.at[expert])
              for expert in range(experts)]
    for copy in copies:
        copy.start()
    token[...] = jnp.zeros_like(token)
    for block in range(blocks):
        count = min(LANES, rows - block * LANES)
        scale_rows[:, pl.ds(block * LANES, count)] = scales[:, block, :count]
    for place in range(n_fsdp):
        taken = [parts[place, group].astype(jnp.float32) for group in range(n_ep)]
        router_rows[:, place * depth:(place + 1) * depth] = (
            jnp.concatenate(taken, axis=0).astype(jnp.bfloat16))
    copies.append(pltpu.make_async_copy(scale_rows, scale_down, small_sem.at[0]))
    copies.append(pltpu.make_async_copy(router_rows, serve_router, small_sem.at[1]))
    for copy in copies[experts:]:
        copy.start()
    for copy in copies:
        copy.wait()


def solution(mesh):
    n_ep, n_fsdp = mesh.shape["ep"], mesh.shape["fsdp"]

    def on_device(master_down, second_down, router_weight, router_gain):
        experts, all_rows, columns = master_down.shape
        rows = all_rows // n_fsdp
        blocks = -(-rows // LANES)
        held = -(-blocks // 8) * 8
        depth, width = router_weight.shape
        dma = pltpu.SemaphoreType.DMA
        vmem, hbm = pl.BlockSpec(memory_space=pltpu.VMEM), pl.BlockSpec(memory_space=pl.ANY)
        n_late = experts - first_late(experts)
        pieces, scales, parts, late = pl.pallas_call(
            functools.partial(exchange, (experts, rows, columns, blocks, n_ep, n_fsdp)),
            out_shape=(
                pltpu.VMEM((experts, rows, columns * n_fsdp), jnp.bfloat16),
                pltpu.VMEM((experts, held, LANES), jnp.float32),
                pltpu.VMEM((n_fsdp, n_ep, width, depth), jnp.bfloat16),
                pltpu.VMEM((max(n_late, 1), 2, rows, columns), jnp.bfloat16),
            ),
            in_specs=[hbm, hbm, vmem, vmem],
            out_specs=(vmem, vmem, vmem, vmem),
            scratch_shapes=[
                pltpu.VMEM((SLOTS, blocks * LANES, columns), jnp.float32),
                pltpu.VMEM((SLOTS, blocks * LANES, columns), jnp.bfloat16),
                pltpu.VMEM((n_fsdp, LANES, columns), jnp.float32),
                pltpu.VMEM((n_fsdp, LANES, columns), jnp.bfloat16),
                pltpu.VMEM((experts * (n_fsdp - 1) - 2 * n_late, rows, columns), jnp.bfloat16),
                pltpu.VMEM((n_fsdp, experts, held, LANES), jnp.float32),
                pltpu.VMEM((n_fsdp, experts, held, LANES), jnp.float32),
                pltpu.VMEM((n_fsdp, experts, held, LANES), jnp.float32),
                pltpu.VMEM((n_fsdp, held, LANES), jnp.float32),
                pltpu.VMEM((n_fsdp, LANES), jnp.float32),
                pltpu.VMEM((n_fsdp, n_fsdp, LANES), jnp.float32),
                pltpu.VMEM((n_fsdp, LANES), jnp.float32),
                dma((2, SLOTS)), dma((2, n_fsdp)),
                dma((experts, n_fsdp)), dma((experts, n_fsdp)),
                dma((experts, n_fsdp)), dma((experts, n_fsdp)),
                dma((experts, n_fsdp)), dma((experts, n_fsdp)),
                dma((n_fsdp,)), dma((n_fsdp,)), dma((n_fsdp,)), dma((n_fsdp,)),
                dma((n_ep,)), dma((n_ep,)), dma((n_fsdp,)), dma((n_fsdp,)),
                pltpu.SemaphoreType.REGULAR,
            ],
            compiler_params=pltpu.CompilerParams(
                collective_id=0, has_side_effects=True, vmem_limit_bytes=32560 * 1024),
        )(master_down, second_down, router_weight.T, router_gain[None, :])
        final_down, scale_down, serve_router, token = pl.pallas_call(
            functools.partial(write, (experts, rows, blocks, n_ep, n_fsdp, depth)),
            out_shape=(
                jax.ShapeDtypeStruct((experts, rows, columns * n_fsdp), jnp.bfloat16),
                jax.ShapeDtypeStruct((experts, rows), jnp.float32),
                jax.ShapeDtypeStruct((n_ep * width, n_fsdp * depth), jnp.bfloat16),
                pltpu.VMEM((8, LANES), jnp.float32),
            ),
            in_specs=[vmem, vmem, vmem],
            out_specs=(hbm, hbm, hbm, vmem),
            scratch_shapes=[
                pltpu.VMEM((experts, rows), jnp.float32),
                pltpu.VMEM((n_ep * width, n_fsdp * depth), jnp.bfloat16),
                dma((experts,)), dma((2,)),
            ],
            compiler_params=pltpu.CompilerParams(vmem_limit_bytes=4 * 1024 * 1024),
        )(pieces, scales, parts)
        if not n_late:
            return final_down, scale_down, serve_router.T
        tail = pl.pallas_call(
            functools.partial(exchange_late, (experts, rows, n_fsdp)),
            out_shape=pltpu.VMEM((n_late, 2, rows, columns), jnp.bfloat16),
            in_specs=[vmem, vmem],
            out_specs=vmem,
            scratch_shapes=[dma((n_late, 2)), dma((n_late, 2))],
            compiler_params=pltpu.CompilerParams(
                collective_id=1, has_side_effects=True, vmem_limit_bytes=1024 * 1024),
        )(late, token)
        final_down = pl.pallas_call(
            functools.partial(write_late, (experts, rows, columns, n_fsdp)),
            out_shape=jax.ShapeDtypeStruct((experts, rows, columns * n_fsdp), jnp.bfloat16),
            in_specs=[hbm, vmem],
            out_specs=hbm,
            scratch_shapes=[dma((n_late, 2))],
            input_output_aliases={0: 0},
            compiler_params=pltpu.CompilerParams(vmem_limit_bytes=1024 * 1024),
        )(final_down, tail)
        return final_down, scale_down, serve_router.T

    placed = (P("ep", None, "fsdp"), P("ep", None, "fsdp"), P("fsdp", "ep"), P("fsdp"))
    return jax.shard_map(
        on_device,
        mesh=mesh,
        in_specs=placed,
        out_specs=(P("ep", "fsdp", None), P("ep", "fsdp"), P()),
        check_vma=False,
    )
```

```python
import functools

import jax
import jax.numpy as jnp
from jax import lax
from jax.experimental import pallas as pl
from jax.experimental.pallas import tpu as pltpu
from jax.sharding import PartitionSpec as P

MESH = pl.DeviceIdType.MESH
LANES = 128
SLOTS = 3
LATE = 1


def partner(me, step, count):
    result, bit = 0, 1
    while bit < count:
        mine, theirs = (me // bit) % 2, (step // bit) % 2
        result = result + bit * (mine + theirs - 2 * mine * theirs)
        bit *= 2
    return result


def over(start, stop, body):
    def run(step, carry):
        body(step)
        return carry
    lax.fori_loop(start, stop, run, 0)


def first_late(experts):
    return experts - min(LATE, experts - 1)


def is_inner(me, n_fsdp):
    quarter = n_fsdp // 4
    return (me >= (2 * quarter - 2)) & (me < 2 * quarter + 2)


def exchange(sizes, master, second, router, gain, final, scales_out, parts, late,
             wide, change, head_wide, head_change, narrow, local_max, pair_max, peer_max, scales, inverse,
             head_max, head_peer, head_inverse,
             load_sem, head_load, rs_send, rs_recv, ag_send, ag_recv, send_sem, recv_sem,
             top_send, top_recv, head_send, head_recv, ep_send, ep_recv, row_send, row_recv,
             pair_send, pair_recv, relay_send, relay_recv, go):
    experts, rows, columns, blocks, n_ep, n_fsdp = sizes
    me, group = lax.axis_index("fsdp"), lax.axis_index("ep")
    inner, side = is_inner(me, n_fsdp), me % 2
    last = rows - (blocks - 1) * LANES
    half = n_fsdp // 2
    lead = min(3, experts)
    passes = [("max", expert) for expert in range(lead)]
    for expert in range(experts):
        passes.append(("scale", expert))
        if lead + expert < experts:
            passes.append(("max", lead + expert))
    fresh = first_late(experts)
    turns = [half if kind == "scale" and expert == 0 else 0 for kind, expert in passes]
    starts = [expert * (n_fsdp - 1) - 2 * max(0, expert - fresh) for expert in range(experts)]
    mine = pl.ds(pl.multiple_of(me * columns, LANES), columns)

    used = pl.ds(0, blocks)

    def rows_of(block):
        return LANES if block < blocks - 1 else last

    def loads(t, expert, step):
        slot, owner = t % SLOTS, partner(me, step, n_fsdp)
        span = pl.ds(pl.multiple_of(owner * rows, 8), rows)
        return (
            pltpu.make_async_copy(
                master.at[expert, span, :], wide.at[slot, pl.ds(0, rows), :], load_sem.at[0, slot]),
            pltpu.make_async_copy(
                second.at[expert, span, :], change.at[slot, pl.ds(0, rows), :], load_sem.at[1, slot]),
        )

    def start_loads(t, expert, step):
        for copy in loads(t, expert, step):
            copy.start()

    def wait_loads(t, expert, step):
        for copy in loads(t, expert, step):
            copy.wait()

    def load_ahead(index, turn):
        expert, ahead = passes[index][1], turn + SLOTS
        if index + 1 < len(passes):
            later = passes[index + 1][1]
            over_end = ahead // n_fsdp
            shift = turns[index] + (turns[index + 1] - turns[index]) * over_end
            start_loads(index * n_fsdp + ahead, expert + (later - expert) * over_end, (ahead + shift) % n_fsdp)
        else:
            @pl.when(ahead < n_fsdp)
            def _():
                start_loads(index * n_fsdp + ahead, expert, (ahead + turns[index]) % n_fsdp)

    def head_loads(step):
        owner = partner(me, step, n_fsdp)
        span = pl.ds(pl.multiple_of(owner * rows, 8), LANES)
        return (
            pltpu.make_async_copy(master.at[0, span, :], head_wide.at[step], head_load.at[0, step]),
            pltpu.make_async_copy(second.at[0, span, :], head_change.at[step], head_load.at[1, step]),
        )

    def to_fsdp(source, target, send, recv, owner):
        return pltpu.make_async_remote_copy(
            src_ref=source, dst_ref=target, send_sem=send, recv_sem=recv,
            device_id={"fsdp": owner}, device_id_type=MESH)

    def top_copy(step):
        return to_fsdp(head_max, head_peer.at[step], top_send.at[step], top_recv.at[step],
                       partner(me, step, n_fsdp))

    def max_copy(expert, step):
        owner = partner(me, step, n_fsdp)
        return to_fsdp(local_max.at[owner // 2, owner % 2, expert, used], peer_max.at[step, expert, used],
                       rs_send.at[expert, step], rs_recv.at[expert, step], owner)

    def scale_copy(expert, step):
        owner = partner(me, step, n_fsdp)
        return to_fsdp(scales.at[me, expert, used], scales.at[me, expert, used],
                       ag_send.at[expert, step], ag_recv.at[expert, step], owner)

    def head_copy(step):
        return to_fsdp(narrow.at[step - 1, pl.ds(0, LANES), :], final.at[0, pl.ds(0, LANES), mine],
                       head_send.at[step], head_recv.at[step], partner(me, step, n_fsdp))

    def piece_copy(expert, step, held_back=False):
        first = LANES if expert == 0 else 0
        span = pl.ds(first, rows - first)
        if held_back:
            source = late.at[expert - fresh, step - (n_fsdp - 2), span, :]
        else:
            source = narrow.at[starts[expert] + step - 1, span, :]
        return to_fsdp(source, final.at[expert, span, mine],
                       send_sem.at[expert, step], recv_sem.at[expert, step], partner(me, step, n_fsdp))

    def row_copy(step):
        return to_fsdp(parts.at[me, group], parts.at[me, group], row_send.at[step], row_recv.at[step],
                       partner(me, step, n_fsdp))

    def column_copy(step):
        return pltpu.make_async_remote_copy(
            src_ref=parts.at[:, group], dst_ref=parts.at[:, group],
            send_sem=ep_send.at[step], recv_sem=ep_recv.at[step],
            device_id={"ep": partner(group, step, n_ep)}, device_id_type=MESH)

    for step in range(n_fsdp):
        for copy in head_loads(step):
            copy.start()
    for t in range(SLOTS):
        start_loads(t, 0, t)
    barrier = pltpu.get_barrier_semaphore()
    for step in range(1, n_fsdp):
        pl.semaphore_signal(barrier, inc=1, device_id={"fsdp": partner(me, step, n_fsdp)}, device_id_type=MESH)
    for step in range(1, n_ep):
        pl.semaphore_signal(barrier, inc=1, device_id={"ep": partner(group, step, n_ep)}, device_id_type=MESH)
    parts[me, group] = (router[...] * gain[...]).astype(jnp.bfloat16)
    local_max[...] = jnp.zeros_like(local_max)
    if last < LANES:
        for slot in range(SLOTS):
            wide[slot, rows:, :] = jnp.zeros((LANES - last, columns), jnp.float32)
            change[slot, rows:, :] = jnp.zeros((LANES - last, columns), jnp.bfloat16)

    def tops(whole):
        entries = jnp.abs(whole)
        top = entries[:, :LANES]
        for first in range(LANES, columns, LANES):
            top = jnp.maximum(top, entries[:, first:first + LANES])
        return jnp.max(top.T, axis=0, keepdims=True)

    def find_head(step):
        for copy in head_loads(step):
            copy.wait()
        whole = head_wide[step] + head_change[step].astype(jnp.float32)
        head_max[pl.ds(partner(me, step, n_fsdp), 1), :] = tops(whole)

    over(0, n_fsdp, find_head)
    pl.semaphore_wait(barrier, n_fsdp + n_ep - 2)
    over(1, n_fsdp, lambda step: top_copy(step).start())
    over(1, n_fsdp, lambda step: row_copy(step).start())

    def merged(slot, block, count):
        span = pl.ds(block * LANES, count)
        return wide[slot, span, :] + change[slot, span, :].astype(jnp.float32)

    def find_max(index, expert, turn):
        t = index * n_fsdp + turn
        wait_loads(t, expert, turn)
        owner, slot = partner(me, turn, n_fsdp), t % SLOTS
        for block in range(1 if expert == 0 else 0, blocks):
            local_max[owner // 2, owner % 2, expert, pl.ds(block, 1), :] = tops(merged(slot, block, LANES))
        load_ahead(index, turn)

    def twice(start, body):
        over(0, (n_fsdp - start) // 2, lambda turn: body(start + 2 * turn))

    def share_scales(expert):
        steps = range(1, n_fsdp) if expert == 0 else range(2, n_fsdp, 2)
        if expert == 0:
            over(1, n_fsdp, lambda step: max_copy(expert, step).wait_recv())
        else:
            twice(2, lambda step: max_copy(expert, step).wait_recv())
        top = local_max[me // 2, side, expert, used]
        for step in steps:
            top = jnp.maximum(top, peer_max[step, expert, used])
        scales[me, expert, used] = top
        if expert == 0:
            scales[me, 0, pl.ds(0, 1), :] = head_max[pl.ds(me, 1), :]
            over(1, n_fsdp, lambda step: scale_copy(expert, step).start())
        else:
            scale_copy(expert, 1).start()
            twice(2, lambda step: scale_copy(expert, step).start())

    def pair_copy(expert):
        return to_fsdp(local_max.at[:, 1 - side, expert, used], pair_max.at[:, expert, used],
                       pair_send.at[expert], pair_recv.at[expert], partner(me, 1, n_fsdp))

    def relay_copy(expert, step):
        source = partner(me, step, n_fsdp)
        return to_fsdp(scales.at[source, expert, used], scales.at[source, expert, used],
                       relay_send.at[expert, step], relay_recv.at[expert, step], partner(me, 1, n_fsdp))

    def start_max(expert):
        if expert == 0:
            over(1, n_fsdp, lambda step: max_copy(expert, step).start())
        else:
            pair_copy(expert).start()

    def join_pair(expert):
        if expert:
            pair_copy(expert).wait_recv()
            for place in range(half):
                local_max[place, side, expert, used] = jnp.maximum(
                    local_max[place, side, expert, used], pair_max[place, expert, used])
            twice(2, lambda step: max_copy(expert, step).start())

    def relay(expert):
        if expert == 0:
            over(1, n_fsdp, lambda step: scale_copy(expert, step).wait_recv())
        else:
            def pass_on(step):
                scale_copy(expert, step).wait_recv()
                relay_copy(expert, step).start()

            twice(2, pass_on)
            scale_copy(expert, 1).wait_recv()

    def settle(expert):
        if expert:
            twice(2, lambda step: relay_copy(expert, step).wait_recv())

    stages, reached = (start_max, join_pair, share_scales, relay, settle), [0] * experts

    def reach(expert, stage):
        if expert < experts:
            while reached[expert] < stage:
                stages[reached[expert]](expert)
                reached[expert] += 1

    def spread(row):
        return jnp.broadcast_to(row, (LANES, LANES)).T

    def scale_block(whole, row, count, expert, block, store):
        factor = spread(row)[:count]
        span = pl.ds(block * LANES, count)
        for first in range(0, columns, LANES):
            part = (whole[:, first:first + LANES] * factor).astype(jnp.bfloat16)
            if store is None:
                final[expert, span, pl.ds(pl.multiple_of(me * columns + first, LANES), LANES)] = part
            else:
                store(span, first, part)

    def scale_head(step):
        source = 0 if step is None else step
        whole = head_wide[source] + head_change[source].astype(jnp.float32)
        row = head_inverse[pl.ds(partner(me, source, n_fsdp), 1), :]
        if step is None:
            scale_block(whole, row, LANES, 0, 0, None)
            return

        def store(span, first, part):
            narrow[step - 1, span, first:first + LANES] = part

        scale_block(whole, row, LANES, 0, 0, store)
        head_copy(step).start()

    def scale_piece(index, expert, kind, turn):
        t = index * n_fsdp + turn

        def to_narrow(span, first, part):
            narrow[starts[expert] + step - 1, span, first:first + LANES] = part

        def to_late(span, first, part):
            late[expert - fresh, step - (n_fsdp - 2), span, first:first + LANES] = part

        step = (turn + turns[index]) % n_fsdp
        wait_loads(t, expert, step)
        owner, slot = partner(me, step, n_fsdp), t % SLOTS
        for block in range(1 if expert == 0 else 0, blocks):
            count = rows_of(block)
            scale_block(merged(slot, block, count), inverse[owner, pl.ds(block, 1), :], count,
                        expert, block, {"own": None, "sent": to_narrow, "late": to_late}[kind])
        load_ahead(index, turn)
        if kind == "sent":
            piece_copy(expert, step).start()
        elif kind == "late" and expert < experts - 1:
            @pl.when(jnp.logical_not(inner))
            def _():
                piece_copy(expert, step, True).start()

    for index, (kind, expert) in enumerate(passes):
        if kind == "max":
            if index == 0:
                over(0, half, functools.partial(find_max, index, expert))
                over(1, n_fsdp, lambda step: top_copy(step).wait())
                top = head_max[...]
                for step in range(1, n_fsdp):
                    top = jnp.maximum(top, head_peer[step])
                head_max[...] = top
                head_inverse[...] = 1.0 / top
                over(half, half + half // 2, scale_head)
                over(half, n_fsdp, functools.partial(find_max, index, expert))
            else:
                over(0, n_fsdp, functools.partial(find_max, index, expert))
                reach(expert - 1, 3 if expert == 1 else 2)
            reach(expert, 1)
            if index >= lead:
                reach(expert, 2)
            if expert == 0:
                over(half + half // 2, n_fsdp - 1, scale_head)
            if expert == min(1, lead - 1):
                over(n_fsdp - 1, n_fsdp, scale_head)
                over(1, half, scale_head)
                scale_head(None)
                over(1, n_fsdp, lambda step: row_copy(step).wait())
                over(1, n_ep, lambda step: column_copy(step).start())
        else:
            reach(expert, 5)
            inverse[...] = 1.0 / scales[:, expert]
            zero = (n_fsdp - turns[index]) % n_fsdp
            stop = n_fsdp - 2 if expert >= fresh else n_fsdp
            if expert == 0 and zero:
                over(0, 1, functools.partial(scale_piece, index, expert, "sent"))
                reach(1, 3)
                reach(2, 2)
                over(1, zero, functools.partial(scale_piece, index, expert, "sent"))
            else:
                over(0, zero, functools.partial(scale_piece, index, expert, "sent"))
            scale_piece(index, expert, "own", zero)
            over(zero + 1, stop, functools.partial(scale_piece, index, expert, "sent"))
            over(stop, n_fsdp, functools.partial(scale_piece, index, expert, "late"))
            reach(expert + 1, 4)
            reach(expert + 2, 3)

    scales_out[...] = scales[me]
    over(1, n_ep, lambda step: column_copy(step).wait())
    over(1, n_fsdp, lambda step: head_copy(step).wait())
    for expert in range(experts):
        if expert == 0:
            over(1, n_fsdp, lambda step: max_copy(expert, step).wait_send())
            over(1, n_fsdp, lambda step: scale_copy(expert, step).wait_send())
        else:
            pair_copy(expert).wait_send()
            scale_copy(expert, 1).wait_send()
            twice(2, lambda step: max_copy(expert, step).wait_send())
            twice(2, lambda step: scale_copy(expert, step).wait_send())
            twice(2, lambda step: relay_copy(expert, step).wait_send())
        over(1, n_fsdp if expert < fresh else n_fsdp - 2, lambda step: piece_copy(expert, step).wait())
    if fresh < experts:
        @pl.when(inner)
        def _():
            for step in range(2, n_fsdp - 2):
                pl.semaphore_signal(go, inc=1, device_id={"fsdp": partner(me, step, n_fsdp)}, device_id_type=MESH)

        @pl.when(jnp.logical_not(inner))
        def _():
            pl.semaphore_wait(go, 4)
            over(n_fsdp - 2, n_fsdp, lambda step: piece_copy(experts - 1, step, True).start())
            for expert in range(fresh, experts):
                over(n_fsdp - 2, n_fsdp, lambda step: piece_copy(expert, step, True).wait())


def exchange_late(sizes, late, written, tail, send_sem, recv_sem):
    experts, rows, n_fsdp = sizes
    me = lax.axis_index("fsdp")
    fresh = first_late(experts)

    @pl.when(is_inner(me, n_fsdp))
    def _():
        barrier = pltpu.get_barrier_semaphore()
        copies = []
        for side in range(2):
            peer = {"fsdp": partner(me, n_fsdp - 2 + side, n_fsdp)}
            pl.semaphore_signal(barrier, inc=1, device_id=peer, device_id_type=MESH)
            for expert in range(fresh, experts):
                piece = (expert - fresh, side)
                copies.append(pltpu.make_async_remote_copy(
                    src_ref=late.at[piece], dst_ref=tail.at[piece],
                    send_sem=send_sem.at[expert - fresh, side], recv_sem=recv_sem.at[expert - fresh, side],
                    device_id=peer, device_id_type=MESH))
        pl.semaphore_wait(barrier, 2)
        for copy in copies:
            copy.start()
        for copy in copies:
            copy.wait()


def write_late(sizes, final_in, tail, final, sem):
    experts, rows, columns, n_fsdp = sizes
    me = lax.axis_index("fsdp")
    fresh = first_late(experts)

    @pl.when(is_inner(me, n_fsdp))
    def _():
        copies = []
        for expert in range(fresh, experts):
            for side in range(2):
                source = partner(me, n_fsdp - 2 + side, n_fsdp)
                copies.append(pltpu.make_async_copy(
                    tail.at[expert - fresh, side],
                    final.at[expert, :, pl.ds(pl.multiple_of(source * columns, LANES), columns)],
                    sem.at[expert - fresh, side]))
        for copy in copies:
            copy.start()
        for copy in copies:
            copy.wait()


def write(sizes, pieces, scales, parts, final, scale_down, serve_router,
          token, scale_rows, router_rows, final_sem, small_sem):
    experts, rows, blocks, n_ep, n_fsdp, depth = sizes
    copies = [pltpu.make_async_copy(pieces.at[expert], final.at[expert], final_sem.at[expert])
              for expert in range(experts)]
    for copy in copies:
        copy.start()
    token[...] = jnp.zeros_like(token)
    for block in range(blocks):
        count = min(LANES, rows - block * LANES)
        scale_rows[:, pl.ds(block * LANES, count)] = scales[:, block, :count]
    for place in range(n_fsdp):
        taken = [parts[place, group].astype(jnp.float32) for group in range(n_ep)]
        router_rows[:, place * depth:(place + 1) * depth] = (
            jnp.concatenate(taken, axis=0).astype(jnp.bfloat16))
    copies.append(pltpu.make_async_copy(scale_rows, scale_down, small_sem.at[0]))
    copies.append(pltpu.make_async_copy(router_rows, serve_router, small_sem.at[1]))
    for copy in copies[experts:]:
        copy.start()
    for copy in copies:
        copy.wait()


def solution(mesh):
    n_ep, n_fsdp = mesh.shape["ep"], mesh.shape["fsdp"]

    def on_device(master_down, second_down, router_weight, router_gain):
        experts, all_rows, columns = master_down.shape
        rows = all_rows // n_fsdp
        blocks = -(-rows // LANES)
        held = -(-blocks // 8) * 8
        depth, width = router_weight.shape
        dma = pltpu.SemaphoreType.DMA
        vmem, hbm = pl.BlockSpec(memory_space=pltpu.VMEM), pl.BlockSpec(memory_space=pl.ANY)
        n_late = experts - first_late(experts)
        pieces, scales, parts, late = pl.pallas_call(
            functools.partial(exchange, (experts, rows, columns, blocks, n_ep, n_fsdp)),
            out_shape=(
                pltpu.VMEM((experts, rows, columns * n_fsdp), jnp.bfloat16),
                pltpu.VMEM((experts, held, LANES), jnp.float32),
                pltpu.VMEM((n_fsdp, n_ep, width, depth), jnp.bfloat16),
                pltpu.VMEM((max(n_late, 1), 2, rows, columns), jnp.bfloat16),
            ),
            in_specs=[hbm, hbm, vmem, vmem],
            out_specs=(vmem, vmem, vmem, vmem),
            scratch_shapes=[
                pltpu.VMEM((SLOTS, blocks * LANES, columns), jnp.float32),
                pltpu.VMEM((SLOTS, blocks * LANES, columns), jnp.bfloat16),
                pltpu.VMEM((n_fsdp, LANES, columns), jnp.float32),
                pltpu.VMEM((n_fsdp, LANES, columns), jnp.bfloat16),
                pltpu.VMEM((experts * (n_fsdp - 1) - 2 * n_late, rows, columns), jnp.bfloat16),
                pltpu.VMEM((n_fsdp // 2, 2, experts, held, LANES), jnp.float32),
                pltpu.VMEM((n_fsdp // 2, experts, held, LANES), jnp.float32),
                pltpu.VMEM((n_fsdp, experts, held, LANES), jnp.float32),
                pltpu.VMEM((n_fsdp, experts, held, LANES), jnp.float32),
                pltpu.VMEM((n_fsdp, held, LANES), jnp.float32),
                pltpu.VMEM((n_fsdp, LANES), jnp.float32),
                pltpu.VMEM((n_fsdp, n_fsdp, LANES), jnp.float32),
                pltpu.VMEM((n_fsdp, LANES), jnp.float32),
                dma((2, SLOTS)), dma((2, n_fsdp)),
                dma((experts, n_fsdp)), dma((experts, n_fsdp)),
                dma((experts, n_fsdp)), dma((experts, n_fsdp)),
                dma((experts, n_fsdp)), dma((experts, n_fsdp)),
                dma((n_fsdp,)), dma((n_fsdp,)), dma((n_fsdp,)), dma((n_fsdp,)),
                dma((n_ep,)), dma((n_ep,)), dma((n_fsdp,)), dma((n_fsdp,)),
                dma((experts,)), dma((experts,)), dma((experts, n_fsdp)), dma((experts, n_fsdp)),
                pltpu.SemaphoreType.REGULAR,
            ],
            compiler_params=pltpu.CompilerParams(
                collective_id=0, has_side_effects=True, vmem_limit_bytes=34 * 1024 * 1024),
        )(master_down, second_down, router_weight.T, router_gain[None, :])
        final_down, scale_down, serve_router, token = pl.pallas_call(
            functools.partial(write, (experts, rows, blocks, n_ep, n_fsdp, depth)),
            out_shape=(
                jax.ShapeDtypeStruct((experts, rows, columns * n_fsdp), jnp.bfloat16),
                jax.ShapeDtypeStruct((experts, rows), jnp.float32),
                jax.ShapeDtypeStruct((n_ep * width, n_fsdp * depth), jnp.bfloat16),
                pltpu.VMEM((8, LANES), jnp.float32),
            ),
            in_specs=[vmem, vmem, vmem],
            out_specs=(hbm, hbm, hbm, vmem),
            scratch_shapes=[
                pltpu.VMEM((experts, rows), jnp.float32),
                pltpu.VMEM((n_ep * width, n_fsdp * depth), jnp.bfloat16),
                dma((experts,)), dma((2,)),
            ],
            compiler_params=pltpu.CompilerParams(vmem_limit_bytes=4 * 1024 * 1024),
        )(pieces, scales, parts)
        if not n_late:
            return final_down, scale_down, serve_router.T
        tail = pl.pallas_call(
            functools.partial(exchange_late, (experts, rows, n_fsdp)),
            out_shape=pltpu.VMEM((n_late, 2, rows, columns), jnp.bfloat16),
            in_specs=[vmem, vmem],
            out_specs=vmem,
            scratch_shapes=[dma((n_late, 2)), dma((n_late, 2))],
            compiler_params=pltpu.CompilerParams(
                collective_id=1, has_side_effects=True, vmem_limit_bytes=1024 * 1024),
        )(late, token)
        final_down = pl.pallas_call(
            functools.partial(write_late, (experts, rows, columns, n_fsdp)),
            out_shape=jax.ShapeDtypeStruct((experts, rows, columns * n_fsdp), jnp.bfloat16),
            in_specs=[hbm, vmem],
            out_specs=hbm,
            scratch_shapes=[dma((n_late, 2))],
            input_output_aliases={0: 0},
            compiler_params=pltpu.CompilerParams(vmem_limit_bytes=1024 * 1024),
        )(final_down, tail)
        return final_down, scale_down, serve_router.T

    placed = (P("ep", None, "fsdp"), P("ep", None, "fsdp"), P("fsdp", "ep"), P("fsdp"))
    return jax.shard_map(
        on_device,
        mesh=mesh,
        in_specs=placed,
        out_specs=(P("ep", "fsdp", None), P("ep", "fsdp"), P()),
        check_vma=False,
    )
```
